32 devices in a mesh: strip: 8 (over z, y), chan: 4 (over x, core).
Axes of the slice: x: 2, y: 2, z: 4, core: 2. Of those that a mesh axis runs over, the one named last changes fastest.
Arguments:
- activations: bfloat16 [64, 128, 1280], P('strip', None, 'chan'), may hold values from -17 to 17
- weight: bfloat16 [9, 1280, 1280], P(None, None, 'chan'), may hold values from -0.0546875 to 0.0546875
- gamma: float32 [1280], replicated, may hold values from 0.25 to 1.75
- beta: float32 [1280], replicated, may hold values from -3 to 3
- group_map: int32 [1280], replicated, may hold values from 0 to 31, as said below
- lengths: int32 [8], P('strip'), may hold values from 1 to 8, 48 in all
- stale_edges: bfloat16 [16, 128, 1280], P('strip', None, 'chan'), may hold values from -6 to 6
- stale_mean: float32 [32], replicated, may hold values from -0.5 to 0.5
- stale_square: float32 [32], replicated, may hold values from 1 to 4
- old_mean: float32 [8, 32], P('strip'), may hold values from -0.5 to 0.5
- old_square: float32 [8, 32], P('strip'), may hold values from 0.5 to 6
Outputs:
- upsampled: bfloat16 [128, 256, 1280], P('strip', None, 'chan')
- new_mean: float32 [32], replicated
- new_square: float32 [32], replicated
The draws below stay inside these ranges and needn't reach their ends.
Inputs may be any that keep to these rules, and one draw needn't show every extreme that they name: `group_map`: every group has exactly 40 channels. The lengths sum to 48, and some strip uses all 8 rows.
All inputs are finite; a program needn't handle non-finite values. No bound on the sum of `lengths` on one device may be relied on, other than what follows from the above.
Results may differ from the reference program's by a relative error of at most 0.0027.
Values may be sent and summed in bfloat16 or wider, within the bound.
A program may use at most 64 MiB of HBM per device.

```python
import math
import jax
import jax.numpy as jnp
import numpy as np
from jax import lax

C = 1280
G = 32
ROWS_DEV = 8
WIDTH = 128
HEIGHT = 64
N_STRIP = 8


def draw_activations(key, part):
    first, second = jax.random.split(key, 2)
    position = jnp.arange(HEIGHT, dtype=jnp.float32) / (HEIGHT - 1)
    noise = jnp.clip(jax.random.normal(first, (HEIGHT, WIDTH, C), jnp.float32), -5.0, 5.0)
    offset = jax.random.uniform(second, (C,), jnp.float32, -1.0, 1.0)
    spread = 1.0 + 2.0 * position
    return (noise * spread[:, None, None] + offset[None, None, :]).astype(jnp.bfloat16)


def draw_group_map(key, part):
    order = jax.random.permutation(key, C)
    return (order // (C // G)).astype(jnp.int32)


def steps_of(rng, shape, cuts, low, top_value):
    level, own = 1.0, jax.random.fold_in(rng, 6)
    for axis_at, blocks in cuts:
        draws = jnp.exp(jax.random.uniform(jax.random.fold_in(own, axis_at), (blocks,), jnp.float32, low / len(cuts), top_value / len(cuts)))
        level = level * jnp.repeat(draws, shape[axis_at] // blocks).reshape([-1 if axis == axis_at else 1 for axis in range(len(shape))])
    return level


def length_profile(count, total, bound, slope):
    loads = [(1 << 20) // math.isqrt(standing ** slope) + 1 for standing in range(2, count + 1)]
    surplus, counts = total - bound - (count - 1), [1] * (count - 1)
    while surplus > 0:
        free = [i for i in range(count - 1) if counts[i] < bound]
        pool, remaining = sum([loads[i] for i in free]), surplus
        for i in free:
            extra = min(bound - counts[i], max(1, remaining * loads[i] // pool), surplus)
            counts[i] = counts[i] + extra
            surplus = surplus - extra
    return np.array([bound] + counts)


def uneven_parts(own_key, amount, total, most, lean):
    if amount == 2:
        one = jax.random.randint(own_key, (), max(1, total - most), min(most, total - 1) + 1)
        return jnp.stack([one, total - one])
    sizes = jnp.asarray(length_profile(amount, total, most, lean), jnp.int32)
    pairs = (amount - 1) // 2
    donor, taker = sizes[1:1 + 2 * pairs:2], sizes[2:2 + 2 * pairs:2]
    margin = jnp.minimum(donor - 1, most - taker)
    shifted = jax.random.randint(jax.random.fold_in(own_key, 1), (pairs,), 0, 1 << 20) % (margin + 1)
    sizes = sizes.at[1:1 + 2 * pairs:2].set(donor - shifted).at[2:2 + 2 * pairs:2].set(taker + shifted)
    return sizes[jax.random.permutation(jax.random.fold_in(own_key, 2), amount)]


def scatter_about(stream_key, extent, scale, bound, pieces=(), kind=jnp.bfloat16):
    drawn = scale * jax.random.normal(stream_key, extent, jnp.float32)
    if pieces:
        drawn = drawn * steps_of(stream_key, extent, pieces, -0.22, 0.18)
    return jnp.clip(drawn, -bound, bound).astype(kind)


def setup_inputs(seed: int = 0) -> dict:
    seeds = jax.random.split(jax.random.key(seed), 12)
    return {
        "activations": draw_activations(jax.random.fold_in(seeds[11], 71), 0),
        "weight": scatter_about(seeds[1], (9, C, C), (9 * C) ** -0.5, 0.0546875, ((2, 4),)),
        "gamma": jnp.clip(1.0 + 0.15 * jax.random.normal(seeds[2], (C,), jnp.float32), 0.25, 1.75),
        "beta": scatter_about(seeds[3], (C,), 0.7, 3.0, (), jnp.float32),
        "group_map": draw_group_map(jax.random.fold_in(seeds[11], 71), 0),
        "lengths": uneven_parts(seeds[5], N_STRIP, N_STRIP * (3 * ROWS_DEV // 4), ROWS_DEV, 2).astype(jnp.int32),
        "stale_edges": scatter_about(seeds[6], (2 * N_STRIP, WIDTH, C), 1.0, 6.0, ((0, 8), (2, 4))),
        "stale_mean": jnp.clip(jax.random.uniform(seeds[7], (G,), jnp.float32, -0.5, 0.5), -0.5, 0.5),
        "stale_square": jnp.clip(jax.random.uniform(seeds[8], (G,), jnp.float32, 1.0, 4.0), 1.0, 4.0),
        "old_mean": jnp.clip(jax.random.uniform(seeds[9], (N_STRIP, G), jnp.float32, -0.5, 0.5) * steps_of(seeds[9], (N_STRIP, G), ((0, 8),), -0.4, 0.0), -0.5, 0.5),
        "old_square": jnp.clip(0.5 + 5.5 * jax.random.uniform(seeds[10], (N_STRIP, G), jnp.float32) ** steps_of(seeds[10], (N_STRIP, G), ((0, 8),), -0.2, 0.2), 0.5, 6.0),
    }


EPS = 1e-05

def reference(activations, weight, gamma, beta, group_map, lengths, stale_edges, stale_mean, stale_square, old_mean, old_square):
    per_group = C // G
    grid = activations.reshape(N_STRIP, ROWS_DEV, WIDTH, C)
    member = (group_map[:, None] == jnp.arange(G, dtype=jnp.int32)[None, :]).astype(jnp.float32)
    used = (jnp.arange(ROWS_DEV, dtype=jnp.int32)[None, :] < lengths[:, None]).astype(jnp.float32)
    values = grid.astype(jnp.float32) * used[:, :, None, None]
    chan_sum = lax.optimization_barrier(jnp.sum(values, axis=(1, 2)))
    chan_sq = lax.optimization_barrier(jnp.sum(values * values, axis=(1, 2)))
    sum_one = lax.optimization_barrier(jnp.sum(chan_sum[:, :, None] * member[None], axis=1))
    sum_two = lax.optimization_barrier(jnp.sum(chan_sq[:, :, None] * member[None], axis=1))
    count = (lengths.astype(jnp.float32) * (WIDTH * per_group))[:, None]
    fresh_mean = sum_one / count
    fresh_square = sum_two / count
    mean_g = stale_mean[None] + fresh_mean - old_mean
    square_g = stale_square[None] + fresh_square - old_square
    var_g = jnp.maximum(square_g - mean_g * mean_g, 0.5 * (fresh_square - fresh_mean * fresh_mean))
    rstd_g = lax.rsqrt(var_g + EPS)
    scale_c = lax.optimization_barrier(jnp.sum(member[None] * rstd_g[:, None, :], axis=2)) * gamma[None]
    shift_c = beta[None] - lax.optimization_barrier(jnp.sum(member[None] * mean_g[:, None, :], axis=2)) * scale_c
    edges = stale_edges.reshape(N_STRIP, 2, WIDTH, C)
    zero_row = jnp.zeros((1, WIDTH, C), jnp.bfloat16)
    upper = jnp.concatenate([zero_row, edges[:-1, 1]], axis=0)
    lower = jnp.concatenate([edges[1:, 0], zero_row], axis=0)

    def one_strip(items):
        strip_x, scale, shift, mask, above, below, length = items
        maskb = mask[:, None, None]
        act = (jax.nn.silu(strip_x.astype(jnp.float32) * scale + shift) * maskb).astype(jnp.bfloat16)
        padded = jnp.concatenate([above[None], act, jnp.zeros((1, WIDTH, C), jnp.bfloat16)], axis=0)
        place = (jnp.arange(ROWS_DEV + 2, dtype=jnp.int32) == length + 1)[:, None, None]
        padded = jnp.where(place, below[None], padded)
        padded = jnp.pad(padded, ((0, 0), (1, 1), (0, 0)))
        total = jnp.zeros((ROWS_DEV * WIDTH, C), jnp.float32)
        for tap in range(9):
            dy, dx = (tap // 3, tap % 3)
            patch = padded[dy:dy + ROWS_DEV, dx:dx + WIDTH].reshape(ROWS_DEV * WIDTH, C)
            total = total + jnp.dot(patch, weight[tap], preferred_element_type=jnp.float32)
        block = (strip_x.astype(jnp.float32) + total.reshape(ROWS_DEV, WIDTH, C)) * maskb
        return block.astype(jnp.bfloat16)
    blocks = lax.map(one_strip, (grid, scale_c, shift_c, used, upper, lower, lengths))
    blocks = blocks.reshape(HEIGHT, WIDTH, C)
    upsampled = jnp.repeat(jnp.repeat(blocks, 2, axis=0), 2, axis=1)
    total_count = float(N_STRIP * (3 * ROWS_DEV // 4) * WIDTH * per_group)
    new_mean = lax.optimization_barrier(jnp.sum(sum_one, axis=0)) / total_count
    new_square = lax.optimization_barrier(jnp.sum(sum_two, axis=0)) / total_count
    return (upsampled, new_mean, new_square)
```

```python
import functools

import jax
import jax.numpy as jnp
from jax import lax
from jax.experimental import pallas as pl
from jax.experimental.pallas import tpu as pltpu
from jax.sharding import PartitionSpec as P

EPS = 1e-05
MESH = pl.DeviceIdType.MESH
F32 = jnp.float32
BF16 = jnp.bfloat16
LANES = 128
HALF = 64


def silu(v):
    return 0.5 * v * (1.0 + jnp.tanh(0.5 * v))


def lane_iota(shape):
    return lax.broadcasted_iota(jnp.int32, shape, len(shape) - 1)


def conv_kernel(
    n_strip,
    n_chan,
    total_count,
    x_hbm,
    w_hbm,
    gamma_ref,
    beta_ref,
    map_ref,
    len_ref,
    edge_hbm,
    smean_ref,
    ssq_ref,
    omean_ref,
    osq_ref,
    out_ref,
    stat_ref,
    xl,
    el,
    ws,
    wr,
    ga,
    gb,
    eb,
    pad,
    st_out,
    st_chan,
    st_strip,
    st_all,
    affine,
    local_sem,
    w_sem,
    send_sem,
    recv_sem,
    edge_send,
    stat_send,
    stat_recv,
    img_send,
    img_recv,
):
    rows, width, local_c = x_hbm.shape
    channels = w_hbm.shape[1]
    groups = smean_ref.shape[1]
    main = local_c // LANES * LANES
    slots = rows + 2
    strip = lax.axis_index("strip")
    me = lax.axis_index("chan")
    n_chips = n_chan // 2
    chip, core = me // 2, me % 2
    partner = chip * 2 + (1 - core)
    up = lax.rem(strip + 1, n_strip)
    down = lax.rem(strip + n_strip - 1, n_strip)
    others = [lax.rem(chip + d, n_chips) * 2 + core for d in range(1, n_chips)]
    sources = [lax.rem(chip + n_chips - d, n_chips) * 2 + core for d in range(1, n_chips)]
    length = len_ref[0]

    x_copy = pltpu.make_async_copy(x_hbm, xl, local_sem.at[0])
    e_copy = pltpu.make_async_copy(edge_hbm, el, local_sem.at[1])
    g_copy = pltpu.make_async_copy(
        x_hbm.at[:, :, pl.ds(0, main)], ga.at[me, pl.ds(1, rows)], local_sem.at[2]
    )
    x_copy.start()
    e_copy.start()
    g_copy.start()
    w_copies = []
    for tap in range(9):
        dy, dx = tap // 3, tap % 3
        for c in range(n_chan):
            for part in range(2):
                if part == 0:
                    src = w_hbm.at[tap, pl.ds(c * local_c, main)]
                    dst = ws.at[dx, pl.ds(dy * channels + c * main, main)]
                else:
                    src = w_hbm.at[tap, pl.ds(c * local_c + main, HALF)]
                    dst = ws.at[dx, pl.ds(dy * channels + n_chan * main + c * HALF, HALF)]
                copy = pltpu.make_async_copy(src, dst, w_sem.at[(tap * n_chan + c) * 2 + part])
                copy.start()
                w_copies.append(copy)

    barrier = pltpu.get_barrier_semaphore()
    greeted = 0
    for d in range(1, n_chan):
        peer = lax.rem(me + d, n_chan)
        pl.semaphore_signal(barrier, inc=1, device_id=(strip, peer), device_id_type=MESH)
        greeted += 1
    for d in range(1, n_strip):
        peer = lax.rem(strip + d, n_strip)
        pl.semaphore_signal(barrier, inc=1, device_id=(peer, me), device_id_type=MESH)
        greeted += 1
    for side in (up, down):
        for c in [partner] + others:
            pl.semaphore_signal(barrier, inc=1, device_id=(side, c), device_id_type=MESH)
            greeted += 1

    lane_h = lane_iota((HALF, LANES))

    def packed(ref, r):
        low = ref[r, pl.ds(0, HALF), pl.ds(main, HALF)].astype(F32)
        high = ref[r, pl.ds(HALF, HALF), pl.ds(main, HALF)].astype(F32)
        return jnp.concatenate([low, high], axis=1).astype(BF16)

    e_copy.wait()
    for k in range(2):
        eb[k] = packed(el, k)
    x_copy.wait()

    def row_sums(r, carry):
        one, two = carry
        gb[me, r + 1] = packed(xl, r)
        value = jnp.where(r < length, xl[r].astype(F32), 0.0).reshape(width // 8, 8, local_c)
        return one + jnp.sum(value, axis=0), two + jnp.sum(value * value, axis=0)

    zero = jnp.zeros((8, local_c), F32)
    one, two = lax.fori_loop(0, rows, row_sums, (zero, zero))
    one = jnp.sum(one, axis=0, keepdims=True)
    two = jnp.sum(two, axis=0, keepdims=True)
    gmap = jnp.broadcast_to(map_ref[...].astype(F32), (8, channels))
    own_map = pltpu.roll(gmap, lax.rem(channels - me * local_c, channels), 1)[0:1, 0:local_c]
    group_id = lax.broadcasted_iota(jnp.int32, (groups, local_c), 0).astype(F32)
    member = (own_map == group_id).astype(F32)
    col_one = jnp.sum(member * one, axis=1, keepdims=True)
    col_two = jnp.sum(member * two, axis=1, keepdims=True)
    eye = (
        lax.broadcasted_iota(jnp.int32, (groups, LANES), 0) == lane_iota((groups, LANES))
    ).astype(F32)
    sub8 = lax.broadcasted_iota(jnp.int32, (8, LANES), 0)

    def as_rows(a, b):
        row_a = jnp.sum(eye * a, axis=0, keepdims=True)
        row_b = jnp.sum(eye * b, axis=0, keepdims=True)
        return jnp.where(sub8 == 0, row_a, jnp.where(sub8 == 1, row_b, 0.0))

    st_out[...] = as_rows(col_one, col_two)
    g_copy.wait()
    pl.semaphore_wait(barrier, greeted)

    sends = []

    def send(src, dst, s_sem, r_sem, device):
        copy = pltpu.make_async_remote_copy(
            src_ref=src, dst_ref=dst, send_sem=s_sem, recv_sem=r_sem,
            device_id=device, device_id_type=MESH,
        )
        copy.start()
        sends.append(copy)
        return copy

    stat_copies = []
    for d in range(1, n_chan):
        peer = lax.rem(me + d, n_chan)
        stat_copies.append(
            send(st_out, st_chan.at[d], stat_send.at[d], stat_recv.at[d], (strip, peer))
        )

    for k, slot, side in ((1, 0, up), (0, slots - 1, down)):
        for kind, c in enumerate([me, partner] + others):
            send(el.at[k, :, pl.ds(0, main)], ga.at[me, slot], edge_send.at[k, kind, 0],
                 recv_sem.at[kind, slot, 0], (side, c))
            send(eb.at[k], gb.at[me, slot], edge_send.at[k, kind, 1],
                 recv_sem.at[kind, slot, 1], (side, c))
    kinds = 1 + n_chips

    def row_copies(slot, kind, c, chan):
        return (
            pltpu.make_async_remote_copy(
                src_ref=ga.at[chan, slot], dst_ref=ga.at[chan, slot],
                send_sem=send_sem.at[kind, slot, 0], recv_sem=recv_sem.at[kind, slot, 0],
                device_id=(strip, c), device_id_type=MESH),
            pltpu.make_async_remote_copy(
                src_ref=gb.at[chan, slot], dst_ref=gb.at[chan, slot],
                send_sem=send_sem.at[kind, slot, 1], recv_sem=recv_sem.at[kind, slot, 1],
                device_id=(strip, c), device_id_type=MESH),
        )

    def start_row(slot, carry):
        for kind, c in enumerate(others):
            for copy in row_copies(slot, 2 + kind, c, me):
                copy.start()
        for copy in row_copies(slot, 1, partner, me):
            copy.start()
        return carry

    lax.fori_loop(1, rows + 1, start_row, 0)

    for copy in w_copies:
        copy.wait()
    block = 256
    wide = jnp.zeros((block, HALF), F32)

    def narrow(k, carry):
        at = pl.ds(pl.multiple_of(k * block, block), block)
        parts = [ws[dx, at, pl.ds(main, HALF)].astype(F32) for dx in range(3)]
        left = jnp.concatenate([parts[0], parts[1]], axis=1)
        right = jnp.concatenate([parts[2], wide], axis=1)
        wr[at, pl.ds(0, LANES)] = left.astype(BF16)
        wr[at, pl.ds(LANES, LANES)] = right.astype(BF16)
        return carry

    lax.fori_loop(0, 3 * channels // block, narrow, 0)

    for copy in stat_copies:
        copy.wait_recv()
    st_chan[0] = st_out[...]
    strip_sum = jnp.zeros((8, LANES), F32)
    for c in range(n_chan):
        strip_sum = strip_sum + st_chan[lax.rem(me - c + n_chan, n_chan)]
    st_strip[...] = strip_sum

    def as_col(row):
        return jnp.sum(eye[:, 0:groups] * row, axis=1, keepdims=True)

    count = length.astype(F32) * (width * (channels // groups))
    fresh_mean = as_col(strip_sum[0:1, 0:groups]) / count
    fresh_sq = as_col(strip_sum[1:2, 0:groups]) / count
    mean_g = as_col(smean_ref[...]) + fresh_mean - as_col(omean_ref[...])
    sq_g = as_col(ssq_ref[...]) + fresh_sq - as_col(osq_ref[...])
    var_g = jnp.maximum(sq_g - mean_g * mean_g, 0.5 * (fresh_sq - fresh_mean * fresh_mean))
    rstd_g = lax.rsqrt(var_g + EPS)
    ids = lax.broadcasted_iota(jnp.int32, (groups, channels), 0).astype(F32)
    member_all = (gmap[0:1] == ids).astype(F32)
    scale = jnp.sum(member_all * rstd_g, axis=0, keepdims=True) * gamma_ref[...]
    shift = beta_ref[...] - jnp.sum(member_all * mean_g, axis=0, keepdims=True) * scale
    lane8 = lane_iota((8, LANES))
    for k, vector in enumerate((scale, shift)):
        vector = jnp.broadcast_to(vector, (8, channels))
        tails = []
        for c in range(n_chan):
            turned = vector if c == 0 else pltpu.roll(vector, channels - c * local_c, 1)
            affine[k, :, pl.ds(c * main, main)] = turned[:, 0:main]
            tails.append(turned[:, main:main + LANES])
        for pair in range(n_chan // 2):
            both = jnp.where(
                lane8 < HALF, tails[2 * pair], pltpu.roll(tails[2 * pair + 1], HALF, 1)
            )
            affine[k, :, pl.ds(n_chan * main + pair * LANES, LANES)] = both

    img_copies = []
    for d in range(1, n_strip):
        peer = lax.rem(strip + d, n_strip)
        img_copies.append(
            send(st_strip, st_all.at[d], img_send.at[d], img_recv.at[d], (peer, me))
        )

    def forward(slot):
        for kind, c in enumerate(sources):
            for copy in row_copies(slot, 2 + kind, c, c):
                copy.wait_recv()
            for copy in row_copies(slot, 1 + n_chips + kind, partner, c):
                copy.start()

    def arrive(slot):
        for copy in row_copies(slot, 1, partner, partner):
            copy.wait_recv()
        for kind, c in enumerate(sources):
            far = c // 2 * 2 + (1 - core)
            for copy in row_copies(slot, 1 + n_chips + kind, partner, far):
                copy.wait_recv()

    def tail_pair(slot, pair):
        even = gb[2 * pair, slot].astype(F32)
        odd = gb[2 * pair + 1, slot].astype(F32)
        top = jnp.where(lane_h < HALF, even, pltpu.roll(odd, HALF, 1))
        bottom = jnp.where(lane_h < HALF, pltpu.roll(even, HALF, 1), odd)
        return jnp.concatenate([top, bottom], axis=0)

    def pieces(slot):
        for c in range(n_chan):
            yield c * main, main, functools.partial(lambda c: ga[c, slot].astype(F32), c)
        for pair in range(n_chan // 2):
            yield (n_chan * main + pair * LANES, LANES,
                   functools.partial(tail_pair, slot, pair))

    for slot in (0, slots - 1):
        forward(slot)
    for slot in (0, slots - 1):
        for copy in row_copies(slot, 0, me, me):
            copy.wait_recv()
        arrive(slot)
    has_above = strip > 0
    has_below = strip < n_strip - 1
    for at, size, load in pieces(0):
        pad[0, :, pl.ds(at, size)] = jnp.where(has_above, load(), 0.0).astype(BF16)
    for at, size, load in pieces(slots - 1):
        below = jnp.where(has_below, load(), 0.0).astype(BF16)
        pad[slots, :, pl.ds(at, size)] = below
        pad[slots - 1, :, pl.ds(at, size)] = jnp.where(
            length + 1 == slots - 1, below.astype(F32), 0.0
        ).astype(BF16)

    def activate(slot):
        forward(slot)
        arrive(slot)
        for at, size, load in pieces(slot):
            span = pl.ds(at, size)
            v = load() * affine[0, 0:1, span] + affine[1, 0:1, span]
            act = jnp.where(slot - 1 < length, silu(v), 0.0)
            below = pad[slots, :, span].astype(F32)
            pad[slot, :, span] = jnp.where(slot == length + 1, below, act).astype(BF16)

    activate(1)
    depth = 2
    m = depth * width
    place = lax.broadcasted_iota(jnp.int32, (m, 1), 0) % width
    lane_m = lane_iota((m, LANES))
    row_of = lax.broadcasted_iota(jnp.int32, (m, 1), 0) // width

    def from_left(y):
        return jnp.where(place == 0, 0.0, pltpu.roll(y, 1, 0))

    def from_right(y):
        return jnp.where(place == width - 1, 0.0, pltpu.roll(y, m - 1, 0))

    def step(t, carry):
        activate(2 * t + 2)

        @pl.when(t < rows // depth - 1)
        def _():
            activate(2 * t + 3)

        first = depth * t
        lhs = jnp.concatenate(
            [pad[pl.ds(first + dy, depth)].reshape(m, channels) for dy in range(3)], axis=1
        )
        dot = functools.partial(jnp.dot, preferred_element_type=F32)
        total = from_left(dot(lhs, ws[0, :, pl.ds(0, main)]))
        total = total + dot(lhs, ws[1, :, pl.ds(0, main)])
        total = total + from_right(dot(lhs, ws[2, :, pl.ds(0, main)]))
        y = dot(lhs, wr[...])
        y0, y2 = y[:, 0:LANES], y[:, LANES:2 * LANES]
        tail = from_left(y0) + pltpu.roll(y0, HALF, 1) + from_right(y2)
        keep = first + row_of < length
        res = xl[pl.ds(first, depth)].reshape(m, local_c).astype(F32)
        head = jnp.where(keep, res[:, 0:main] + total, 0.0).astype(BF16)
        last = jnp.where(keep, res[:, main:local_c] + tail[:, 0:HALF], 0.0).astype(BF16)
        out_ref[pl.ds(first, depth), :, pl.ds(0, main)] = head.reshape(depth, width, main)
        out_ref[pl.ds(first, depth), :, pl.ds(main, HALF)] = last.reshape(depth, width, HALF)
        return carry

    lax.fori_loop(0, rows // depth, step, 0)

    for copy in img_copies:
        copy.wait_recv()
    st_all[0] = st_strip[...]
    image = jnp.zeros((8, LANES), F32)
    for i in range(n_strip):
        image = image + st_all[lax.rem(strip - i + n_strip, n_strip)]
    stat_ref[...] = image / total_count

    for copy in sends:
        copy.wait_send()

    def drain(slot, carry):
        for kind in range(1, 2 + n_chips - 1):
            for copy in row_copies(slot, kind, partner, me):
                copy.wait_send()
        return carry

    def drain_forward(slot, carry):
        for kind in range(1 + n_chips, 2 * n_chips):
            for copy in row_copies(slot, kind, partner, me):
                copy.wait_send()
        return carry

    lax.fori_loop(1, rows + 1, drain, 0)
    lax.fori_loop(0, slots, drain_forward, 0)


def upsample_kernel(block_ref, stat_ref, out_ref, mean_ref, square_ref):
    _, width, _ = block_ref.shape
    target = lax.broadcasted_iota(jnp.int32, (2 * width, width), 0) // 2
    source = lax.broadcasted_iota(jnp.int32, (2 * width, width), 1)
    twice = (target == source).astype(F32).astype(BF16)
    wide = jnp.dot(twice, block_ref[0], preferred_element_type=F32).astype(BF16)
    out_ref[0] = wide
    out_ref[1] = wide
    groups = mean_ref.shape[1]
    mean_ref[...] = stat_ref[0:1, 0:groups]
    square_ref[...] = stat_ref[1:2, 0:groups]


def per_device(
    n_strip,
    n_chan,
    activations,
    weight,
    gamma,
    beta,
    group_map,
    lengths,
    stale_edges,
    stale_mean,
    stale_square,
    old_mean,
    old_square,
):
    rows, width, local_c = activations.shape
    channels = weight.shape[1]
    groups = stale_mean.shape[0]
    main = local_c // LANES * LANES
    slots = rows + 2
    n_chips = n_chan // 2
    kinds = 2 * n_chips
    total_count = float(n_strip * (3 * rows // 4) * width * (channels // groups))
    vmem = pl.BlockSpec(memory_space=pltpu.VMEM)
    hbm = pl.BlockSpec(memory_space=pl.ANY)
    dma = pltpu.SemaphoreType.DMA
    block, stat = pl.pallas_call(
        functools.partial(conv_kernel, n_strip, n_chan, total_count),
        out_shape=(
            jax.ShapeDtypeStruct((rows, width, local_c), BF16),
            jax.ShapeDtypeStruct((8, LANES), F32),
        ),
        in_specs=[hbm, hbm, vmem, vmem, vmem, pl.BlockSpec(memory_space=pltpu.SMEM), hbm,
                  vmem, vmem, vmem, vmem],
        out_specs=(vmem, vmem),
        scratch_shapes=[
            pltpu.VMEM((rows, width, local_c), BF16),
            pltpu.VMEM((2, width, local_c), BF16),
            pltpu.VMEM((3, 3 * channels, local_c), BF16),
            pltpu.VMEM((3 * channels, 2 * LANES), BF16),
            pltpu.VMEM((n_chan, slots, width, main), BF16),
            pltpu.VMEM((n_chan, slots, HALF, LANES), BF16),
            pltpu.VMEM((2, HALF, LANES), BF16),
            pltpu.VMEM((slots + 1, width, channels), BF16),
            pltpu.VMEM((8, LANES), F32),
            pltpu.VMEM((n_chan, 8, LANES), F32),
            pltpu.VMEM((8, LANES), F32),
            pltpu.VMEM((n_strip, 8, LANES), F32),
            pltpu.VMEM((2, 8, channels), F32),
            dma((3,)),
            dma((9 * n_chan * 2,)),
            dma((kinds, slots, 2)),
            dma((kinds, slots, 2)),
            dma((2, 1 + n_chips, 2)),
            dma((n_chan,)),
            dma((n_chan,)),
            dma((n_strip,)),
            dma((n_strip,)),
        ],
        compiler_params=pltpu.CompilerParams(
            collective_id=0, has_side_effects=True, vmem_limit_bytes=56 * 2**20
        ),
        name="conv",
    )(
        activations,
        weight,
        gamma.reshape(1, channels),
        beta.reshape(1, channels),
        group_map.reshape(1, channels),
        lengths,
        stale_edges,
        stale_mean.reshape(1, groups),
        stale_square.reshape(1, groups),
        old_mean,
        old_square,
    )
    whole = pl.BlockSpec((1, groups), lambda r: (0, 0))
    upsampled, mean, square = pl.pallas_call(
        upsample_kernel,
        grid=(rows,),
        out_shape=(
            jax.ShapeDtypeStruct((2 * rows, 2 * width, local_c), BF16),
            jax.ShapeDtypeStruct((1, groups), F32),
            jax.ShapeDtypeStruct((1, groups), F32),
        ),
        in_specs=[
            pl.BlockSpec((1, width, local_c), lambda r: (r, 0, 0)),
            pl.BlockSpec((8, LANES), lambda r: (0, 0)),
        ],
        out_specs=(pl.BlockSpec((2, 2 * width, local_c), lambda r: (r, 0, 0)), whole, whole),
        name="upsample",
    )(block, stat)
    return upsampled, mean.reshape(groups), square.reshape(groups)


def solution(mesh):
    in_specs = (
        P("strip", None, "chan"),
        P(None, None, "chan"),
        P(),
        P(),
        P(),
        P("strip"),
        P("strip", None, "chan"),
        P(),
        P(),
        P("strip", None),
        P("strip", None),
    )
    out_specs = (P("strip", None, "chan"), P(), P())
    body = functools.partial(per_device, mesh.shape["strip"], mesh.shape["chan"])
    return jax.shard_map(
        body, mesh=mesh, in_specs=in_specs, out_specs=out_specs, check_vma=False
    )
```

```python
import functools

import jax
import jax.numpy as jnp
from jax import lax
from jax.experimental import pallas as pl
from jax.experimental.pallas import tpu as pltpu
from jax.sharding import PartitionSpec as P

EPS = 1e-05
MESH = pl.DeviceIdType.MESH
F32 = jnp.float32
BF16 = jnp.bfloat16
LANES = 128


def spread(row):
    return jnp.transpose(jnp.broadcast_to(row, (LANES, LANES)))


def lane_iota(shape):
    return lax.broadcasted_iota(jnp.int32, shape, len(shape) - 1)


def conv_kernel(
    n_strip,
    n_chan,
    total_count,
    x_hbm,
    w_hbm,
    gamma_ref,
    beta_ref,
    map_ref,
    len_ref,
    edge_hbm,
    smean_ref,
    ssq_ref,
    omean_ref,
    osq_ref,
    out_ref,
    stat_ref,
    xl,
    el,
    ws,
    ga,
    pad,
    st_out,
    st_chan,
    st_strip,
    st_all,
    affine,
    local_sem,
    w_sem,
    send_sem,
    recv_sem,
    edge_send,
    stat_send,
    stat_recv,
    img_send,
    img_recv,
):
    rows, local_c, width = x_hbm.shape
    channels = w_hbm.shape[2]
    groups = smean_ref.shape[1]
    slots = rows + 2
    strip = lax.axis_index("strip")
    me = lax.axis_index("chan")
    n_chips = n_chan // 2
    chip, core = me // 2, me % 2
    partner = chip * 2 + (1 - core)
    up = lax.rem(strip + 1, n_strip)
    down = lax.rem(strip + n_strip - 1, n_strip)
    others = [lax.rem(chip + d, n_chips) * 2 + core for d in range(1, n_chips)]
    sources = [lax.rem(chip + n_chips - d, n_chips) * 2 + core for d in range(1, n_chips)]
    length = len_ref[0]

    x_copy = pltpu.make_async_copy(x_hbm, xl, local_sem.at[0])
    e_copy = pltpu.make_async_copy(edge_hbm, el, local_sem.at[1])
    g_copy = pltpu.make_async_copy(x_hbm, ga.at[me, pl.ds(1, rows)], local_sem.at[2])
    x_copy.start()
    e_copy.start()
    g_copy.start()
    w_copies = []
    for dy in range(3):
        taps = pl.ds(3 * dy, 3)
        copy = pltpu.make_async_copy(w_hbm.at[taps], ws.at[taps], w_sem.at[dy])
        copy.start()
        w_copies.append(copy)

    barrier = pltpu.get_barrier_semaphore()
    greeted = 0
    for d in range(1, n_chan):
        peer = lax.rem(me + d, n_chan)
        pl.semaphore_signal(barrier, inc=1, device_id=(strip, peer), device_id_type=MESH)
        greeted += 1
    for d in range(1, n_strip):
        peer = lax.rem(strip + d, n_strip)
        pl.semaphore_signal(barrier, inc=1, device_id=(peer, me), device_id_type=MESH)
        greeted += 1
    for side in (up, down):
        for c in [partner] + others:
            pl.semaphore_signal(barrier, inc=1, device_id=(side, c), device_id_type=MESH)
            greeted += 1

    e_copy.wait()
    x_copy.wait()

    def row_sums(r, carry):
        one, two = carry
        value = jnp.where(r < length, xl[r].astype(F32), 0.0)
        return one + value, two + value * value

    zero = jnp.zeros((local_c, width), F32)
    one, two = lax.fori_loop(0, rows, row_sums, (zero, zero))
    one = jnp.sum(one, axis=1, keepdims=True)
    two = jnp.sum(two, axis=1, keepdims=True)
    gmap = jnp.broadcast_to(map_ref[...].reshape(1, channels).astype(F32), (8, channels))
    own_map = pltpu.roll(gmap, lax.rem(channels - me * local_c, channels), 1)[0:1]
    blocks = -(-local_c // LANES)
    own_map = jnp.concatenate(
        [spread(own_map[:, k * LANES:(k + 1) * LANES]) for k in range(blocks)], axis=0
    )[0:local_c]
    member = (own_map == lane_iota((local_c, LANES)).astype(F32)).astype(F32)
    row_one = jnp.sum(member * one, axis=0, keepdims=True)
    row_two = jnp.sum(member * two, axis=0, keepdims=True)
    eye = (
        lax.broadcasted_iota(jnp.int32, (groups, LANES), 0) == lane_iota((groups, LANES))
    ).astype(F32)
    sub8 = lax.broadcasted_iota(jnp.int32, (8, LANES), 0)
    st_out[...] = jnp.where(sub8 == 0, row_one, jnp.where(sub8 == 1, row_two, 0.0))
    g_copy.wait()
    pl.semaphore_wait(barrier, greeted)

    sends = []

    def send(src, dst, s_sem, r_sem, device):
        copy = pltpu.make_async_remote_copy(
            src_ref=src, dst_ref=dst, send_sem=s_sem, recv_sem=r_sem,
            device_id=device, device_id_type=MESH,
        )
        copy.start()
        sends.append(copy)
        return copy

    stat_copies = []
    for d in range(1, n_chan):
        peer = lax.rem(me + d, n_chan)
        stat_copies.append(
            send(st_out, st_chan.at[d], stat_send.at[d], stat_recv.at[d], (strip, peer))
        )

    for k, slot, side in ((1, 0, up), (0, slots - 1, down)):
        for kind, c in enumerate([me, partner] + others):
            send(el.at[k], ga.at[me, slot], edge_send.at[k, kind],
                 recv_sem.at[kind, slot], (side, c))

    def row_copy(slot, kind, c, chan):
        return pltpu.make_async_remote_copy(
            src_ref=ga.at[chan, slot], dst_ref=ga.at[chan, slot],
            send_sem=send_sem.at[kind, slot], recv_sem=recv_sem.at[kind, slot],
            device_id=(strip, c), device_id_type=MESH,
        )

    def start_row(slot, carry):
        for kind, c in enumerate(others):
            row_copy(slot, 2 + kind, c, me).start()
        row_copy(slot, 1, partner, me).start()
        return carry

    lax.fori_loop(1, rows + 1, start_row, 0)

    for copy in stat_copies:
        copy.wait_recv()
    st_chan[0] = st_out[...]
    strip_sum = jnp.zeros((8, LANES), F32)
    for c in range(n_chan):
        strip_sum = strip_sum + st_chan[lax.rem(me - c + n_chan, n_chan)]
    st_strip[...] = strip_sum

    def as_col(row):
        return jnp.sum(eye[:, 0:groups] * row, axis=1, keepdims=True)

    count = length.astype(F32) * (width * (channels // groups))
    fresh_mean = as_col(strip_sum[0:1, 0:groups]) / count
    fresh_sq = as_col(strip_sum[1:2, 0:groups]) / count
    mean_g = as_col(smean_ref[...]) + fresh_mean - as_col(omean_ref[...])
    sq_g = as_col(ssq_ref[...]) + fresh_sq - as_col(osq_ref[...])
    var_g = jnp.maximum(sq_g - mean_g * mean_g, 0.5 * (fresh_sq - fresh_mean * fresh_mean))
    rstd_g = lax.rsqrt(var_g + EPS)
    ids = lax.broadcasted_iota(jnp.int32, (groups, channels), 0).astype(F32)
    member_all = (gmap[0:1] == ids).astype(F32)
    scale = jnp.sum(member_all * rstd_g, axis=0, keepdims=True) * gamma_ref[...].reshape(1, channels)
    shift = beta_ref[...].reshape(1, channels) - (
        jnp.sum(member_all * mean_g, axis=0, keepdims=True) * scale
    )
    for k, vector in enumerate((scale, shift)):
        for j in range(channels // LANES):
            span = slice(j * LANES, (j + 1) * LANES)
            affine[k, span, :] = spread(0.5 * vector[:, span])

    img_copies = []
    for d in range(1, n_strip):
        peer = lax.rem(strip + d, n_strip)
        img_copies.append(
            send(st_strip, st_all.at[d], img_send.at[d], img_recv.at[d], (peer, me))
        )

    def forward(slot):
        for kind, c in enumerate(sources):
            row_copy(slot, 2 + kind, c, c).wait_recv()
            row_copy(slot, 1 + n_chips + kind, partner, c).start()

    def arrive(slot):
        row_copy(slot, 1, partner, partner).wait_recv()
        for kind, c in enumerate(sources):
            far = c // 2 * 2 + (1 - core)
            row_copy(slot, 1 + n_chips + kind, partner, far).wait_recv()

    for slot in (0, slots - 1):
        forward(slot)
    for slot in (0, slots - 1):
        row_copy(slot, 0, me, me).wait_recv()
        arrive(slot)
    has_above = strip > 0
    has_below = strip < n_strip - 1
    for c in range(n_chan):
        span = pl.ds(c * local_c, local_c)
        pad[0, span] = jnp.where(has_above, ga[c, 0].astype(F32), 0.0).astype(BF16)
        below = jnp.where(has_below, ga[c, slots - 1].astype(F32), 0.0)
        pad[slots, span] = below.astype(BF16)
        pad[slots - 1, span] = jnp.where(length + 1 == slots - 1, below, 0.0).astype(BF16)

    def activate(slot):
        forward(slot)
        arrive(slot)
        for c in range(n_chan):
            span = pl.ds(c * local_c, local_c)
            h = ga[c, slot].astype(F32) * affine[0, span] + affine[1, span]
            act = jnp.where(slot - 1 < length, h + h * jnp.tanh(h), 0.0)
            below = pad[slots, span].astype(F32)
            pad[slot, span] = jnp.where(slot == length + 1, below, act).astype(BF16)

    for copy in w_copies:
        copy.wait()
    activate(1)
    depth = 2
    place = lane_iota((local_c, width))

    def from_left(y):
        return jnp.where(place == 0, 0.0, pltpu.roll(y, 1, 1))

    def from_right(y):
        return jnp.where(place == width - 1, 0.0, pltpu.roll(y, width - 1, 1))

    def step(t, carry):
        activate(2 * t + 2)

        @pl.when(t < rows // depth - 1)
        def _():
            activate(2 * t + 3)

        first = depth * t
        rhs = jnp.concatenate(
            [
                jnp.concatenate([pad[first + dy + k] for k in range(depth)], axis=1)
                for dy in range(3)
            ],
            axis=0,
        )
        y = []
        for dx in range(3):
            lhs = jnp.concatenate([ws[3 * dy + dx] for dy in range(3)], axis=1)
            y.append(jnp.dot(lhs, rhs, preferred_element_type=F32))
        for k in range(depth):
            span = slice(k * width, (k + 1) * width)
            total = from_left(y[0][:, span]) + y[1][:, span] + from_right(y[2][:, span])
            block = xl[first + k].astype(F32) + total
            out_ref[first + k] = jnp.where(first + k < length, block, 0.0).astype(BF16)
        return carry

    lax.fori_loop(0, rows // depth, step, 0)

    for copy in img_copies:
        copy.wait_recv()
    st_all[0] = st_strip[...]
    image = jnp.zeros((8, LANES), F32)
    for i in range(n_strip):
        image = image + st_all[lax.rem(strip - i + n_strip, n_strip)]
    stat_ref[...] = image / total_count

    for copy in sends:
        copy.wait_send()

    def drain(slot, carry):
        for kind in range(1, 2 + n_chips - 1):
            row_copy(slot, kind, partner, me).wait_send()
        return carry

    def drain_forward(slot, carry):
        for kind in range(1 + n_chips, 2 * n_chips):
            row_copy(slot, kind, partner, me).wait_send()
        return carry

    lax.fori_loop(1, rows + 1, drain, 0)
    lax.fori_loop(0, slots, drain_forward, 0)


def upsample_kernel(block_ref, stat_ref, out_ref, mean_ref, square_ref):
    depth, _, width = block_ref.shape
    source = lax.broadcasted_iota(jnp.int32, (width, 2 * width), 0)
    target = lax.broadcasted_iota(jnp.int32, (width, 2 * width), 1) // 2
    twice = (target == source).astype(F32).astype(BF16)
    for r in range(depth):
        wide = jnp.dot(block_ref[r], twice, preferred_element_type=F32).astype(BF16)
        out_ref[2 * r] = wide
        out_ref[2 * r + 1] = wide
    groups = mean_ref.shape[1]
    mean_ref[...] = stat_ref[0:1, 0:groups]
    square_ref[...] = stat_ref[1:2, 0:groups]


def per_device(
    n_strip,
    n_chan,
    activations,
    weight,
    gamma,
    beta,
    group_map,
    lengths,
    stale_edges,
    stale_mean,
    stale_square,
    old_mean,
    old_square,
):
    rows, width, local_c = activations.shape
    channels = weight.shape[1]
    groups = stale_mean.shape[0]
    slots = rows + 2
    n_chips = n_chan // 2
    kinds = 2 * n_chips
    total_count = float(n_strip * (3 * rows // 4) * width * (channels // groups))
    vmem = pl.BlockSpec(memory_space=pltpu.VMEM)
    hbm = pl.BlockSpec(memory_space=pl.ANY)
    dma = pltpu.SemaphoreType.DMA
    block, stat = pl.pallas_call(
        functools.partial(conv_kernel, n_strip, n_chan, total_count),
        out_shape=(
            jax.ShapeDtypeStruct((rows, local_c, width), BF16),
            jax.ShapeDtypeStruct((8, LANES), F32),
        ),
        in_specs=[hbm, hbm, vmem, vmem, vmem, pl.BlockSpec(memory_space=pltpu.SMEM), hbm,
                  vmem, vmem, vmem, vmem],
        out_specs=(vmem, vmem),
        scratch_shapes=[
            pltpu.VMEM((rows, local_c, width), BF16),
            pltpu.VMEM((2, local_c, width), BF16),
            pltpu.VMEM((9, local_c, channels), BF16),
            pltpu.VMEM((n_chan, slots, local_c, width), BF16),
            pltpu.VMEM((slots + 1, channels, width), BF16),
            pltpu.VMEM((8, LANES), F32),
            pltpu.VMEM((n_chan, 8, LANES), F32),
            pltpu.VMEM((8, LANES), F32),
            pltpu.VMEM((n_strip, 8, LANES), F32),
            pltpu.VMEM((2, channels, width), F32),
            dma((3,)),
            dma((3,)),
            dma((kinds, slots)),
            dma((kinds, slots)),
            dma((2, 1 + n_chips)),
            dma((n_chan,)),
            dma((n_chan,)),
            dma((n_strip,)),
            dma((n_strip,)),
        ],
        compiler_params=pltpu.CompilerParams(
            collective_id=0, has_side_effects=True, vmem_limit_bytes=56 * 2**20
        ),
        name="conv",
    )(
        jnp.transpose(activations, (0, 2, 1)),
        jnp.transpose(weight, (0, 2, 1)),
        gamma,
        beta,
        group_map,
        lengths,
        jnp.transpose(stale_edges, (0, 2, 1)),
        stale_mean.reshape(1, groups),
        stale_square.reshape(1, groups),
        old_mean,
        old_square,
    )
    whole = pl.BlockSpec((1, groups), lambda r: (0, 0))
    upsampled, mean, square = pl.pallas_call(
        upsample_kernel,
        grid=(rows // 2,),
        out_shape=(
            jax.ShapeDtypeStruct((2 * rows, local_c, 2 * width), BF16),
            jax.ShapeDtypeStruct((1, groups), F32),
            jax.ShapeDtypeStruct((1, groups), F32),
        ),
        in_specs=[
            pl.BlockSpec((2, local_c, width), lambda r: (r, 0, 0)),
            pl.BlockSpec((8, LANES), lambda r: (0, 0)),
        ],
        out_specs=(pl.BlockSpec((4, local_c, 2 * width), lambda r: (r, 0, 0)), whole, whole),
        name="upsample",
    )(block, stat)
    upsampled = jnp.transpose(upsampled, (0, 2, 1))
    return upsampled, mean.reshape(groups), square.reshape(groups)


def solution(mesh):
    in_specs = (
        P("strip", None, "chan"),
        P(None, None, "chan"),
        P(),
        P(),
        P(),
        P("strip"),
        P("strip", None, "chan"),
        P(),
        P(),
        P("strip", None),
        P("strip", None),
    )
    out_specs = (P("strip", None, "chan"), P(), P())
    body = functools.partial(per_device, mesh.shape["strip"], mesh.shape["chan"])
    return jax.shard_map(
        body, mesh=mesh, in_specs=in_specs, out_specs=out_specs, check_vma=False
    )
```

```python
import functools

import jax
import jax.numpy as jnp
from jax import lax
from jax.experimental import pallas as pl
from jax.experimental.pallas import tpu as pltpu
from jax.sharding import PartitionSpec as P

EPS = 1e-05
MESH = pl.DeviceIdType.MESH
F32 = jnp.float32
BF16 = jnp.bfloat16
LANES = 128
CHUNK = 64
WINDOW = 5


def spread(row):
    return jnp.transpose(jnp.broadcast_to(row, (LANES, LANES)))


def lane_iota(shape):
    return lax.broadcasted_iota(jnp.int32, shape, len(shape) - 1)


def conv_kernel(
    n_strip,
    n_chan,
    total_count,
    x_hbm,
    w_hbm,
    gamma_ref,
    beta_ref,
    map_ref,
    len_ref,
    edge_hbm,
    smean_ref,
    ssq_ref,
    omean_ref,
    osq_ref,
    out_ref,
    stat_ref,
    xl,
    el,
    ws,
    ga,
    pad,
    st_out,
    st_chan,
    st_strip,
    st_all,
    affine,
    local_sem,
    w_sem,
    send_sem,
    recv_sem,
    edge_send,
    stat_send,
    stat_recv,
    img_send,
    img_recv,
):
    rows, local_c, width = x_hbm.shape
    channels = w_hbm.shape[2]
    groups = smean_ref.shape[1]
    slots = rows + 2
    strip = lax.axis_index("strip")
    me = lax.axis_index("chan")
    n_chips = n_chan // 2
    chip, core = me // 2, me % 2
    partner = chip * 2 + (1 - core)
    up = lax.rem(strip + 1, n_strip)
    down = lax.rem(strip + n_strip - 1, n_strip)
    others = [lax.rem(chip + d, n_chips) * 2 + core for d in range(1, n_chips)]
    sources = [lax.rem(chip + n_chips - d, n_chips) * 2 + core for d in range(1, n_chips)]
    length = len_ref[0]

    x_copy = pltpu.make_async_copy(x_hbm, xl, local_sem.at[0])
    e_copy = pltpu.make_async_copy(edge_hbm, el, local_sem.at[1])
    g_copy = pltpu.make_async_copy(x_hbm, ga.at[me, pl.ds(1, rows)], local_sem.at[2])
    x_copy.start()
    e_copy.start()
    g_copy.start()
    w_copies = []
    for dy in range(3):
        taps = pl.ds(3 * dy, 3)
        copy = pltpu.make_async_copy(w_hbm.at[taps], ws.at[taps], w_sem.at[dy])
        copy.start()
        w_copies.append(copy)

    barrier = pltpu.get_barrier_semaphore()
    greeted = 0
    for d in range(1, n_chan):
        peer = lax.rem(me + d, n_chan)
        pl.semaphore_signal(barrier, inc=1, device_id=(strip, peer), device_id_type=MESH)
        greeted += 1
    for d in range(1, n_strip):
        peer = lax.rem(strip + d, n_strip)
        pl.semaphore_signal(barrier, inc=1, device_id=(peer, me), device_id_type=MESH)
        greeted += 1
    for side in (up, down):
        for c in [partner] + others:
            pl.semaphore_signal(barrier, inc=1, device_id=(side, c), device_id_type=MESH)
            greeted += 1

    e_copy.wait()
    pl.semaphore_wait(barrier, greeted)

    sends = []

    def send(src, dst, s_sem, r_sem, device):
        copy = pltpu.make_async_remote_copy(
            src_ref=src, dst_ref=dst, send_sem=s_sem, recv_sem=r_sem,
            device_id=device, device_id_type=MESH,
        )
        copy.start()
        sends.append(copy)
        return copy

    for k, slot, side in ((1, 0, up), (0, slots - 1, down)):
        for kind, c in enumerate([me, partner] + others):
            send(el.at[k], ga.at[me, slot], edge_send.at[k, kind],
                 recv_sem.at[kind, slot], (side, c))

    x_copy.wait()
    sums_one, sums_two = [], []
    for at in range(0, local_c, CHUNK):
        one = two = jnp.zeros((CHUNK, width), F32)
        for r in range(rows):
            value = jnp.where(r < length, xl[r, pl.ds(at, CHUNK)].astype(F32), 0.0)
            one, two = one + value, two + value * value
        sums_one.append(jnp.sum(one, axis=1, keepdims=True))
        sums_two.append(jnp.sum(two, axis=1, keepdims=True))
    one = jnp.concatenate(sums_one, axis=0)
    two = jnp.concatenate(sums_two, axis=0)
    gmap = jnp.broadcast_to(map_ref[...].reshape(1, channels).astype(F32), (8, channels))
    own_map = pltpu.roll(gmap, lax.rem(channels - me * local_c, channels), 1)[0:1]
    blocks = -(-local_c // LANES)
    own_map = jnp.concatenate(
        [spread(own_map[:, k * LANES:(k + 1) * LANES]) for k in range(blocks)], axis=0
    )[0:local_c]
    member = (own_map == lane_iota((local_c, LANES)).astype(F32)).astype(F32)
    row_one = jnp.sum(member * one, axis=0, keepdims=True)
    row_two = jnp.sum(member * two, axis=0, keepdims=True)
    eye = (
        lax.broadcasted_iota(jnp.int32, (groups, LANES), 0) == lane_iota((groups, LANES))
    ).astype(F32)
    sub8 = lax.broadcasted_iota(jnp.int32, (8, LANES), 0)
    st_out[...] = jnp.where(sub8 == 0, row_one, jnp.where(sub8 == 1, row_two, 0.0))
    stat_copies = []
    for d in range(1, n_chan):
        peer = lax.rem(me + d, n_chan)
        stat_copies.append(
            send(st_out, st_chan.at[d], stat_send.at[d], stat_recv.at[d], (strip, peer))
        )

    def row_copy(slot, kind, c, chan):
        return pltpu.make_async_remote_copy(
            src_ref=ga.at[chan, slot], dst_ref=ga.at[chan, slot],
            send_sem=send_sem.at[kind, slot], recv_sem=recv_sem.at[kind, slot],
            device_id=(strip, c), device_id_type=MESH,
        )

    g_copy.wait()
    def start_row(slot, carry):
        for kind, c in enumerate(others):
            row_copy(slot, 2 + kind, c, me).start()
        row_copy(slot, 1, partner, me).start()
        return carry

    lax.fori_loop(1, min(WINDOW, rows) + 1, start_row, 0)

    def forward(slot):
        for kind, c in enumerate(sources):
            row_copy(slot, 2 + kind, c, c).wait_recv()
            row_copy(slot, 1 + n_chips + kind, partner, c).start()

    def arrive(slot):
        row_copy(slot, 1, partner, partner).wait_recv()
        for kind, c in enumerate(sources):
            far = c // 2 * 2 + (1 - core)
            row_copy(slot, 1 + n_chips + kind, partner, far).wait_recv()

    for slot in (0, slots - 1):
        forward(slot)

    for copy in stat_copies:
        copy.wait_recv()
    st_chan[0] = st_out[...]
    strip_sum = jnp.zeros((8, LANES), F32)
    for c in range(n_chan):
        strip_sum = strip_sum + st_chan[lax.rem(me - c + n_chan, n_chan)]
    st_strip[...] = strip_sum

    def as_col(row):
        return jnp.sum(eye[:, 0:groups] * row, axis=1, keepdims=True)

    count = length.astype(F32) * (width * (channels // groups))
    fresh_mean = as_col(strip_sum[0:1, 0:groups]) / count
    fresh_sq = as_col(strip_sum[1:2, 0:groups]) / count
    mean_g = as_col(smean_ref[...]) + fresh_mean - as_col(omean_ref[...])
    sq_g = as_col(ssq_ref[...]) + fresh_sq - as_col(osq_ref[...])
    var_g = jnp.maximum(sq_g - mean_g * mean_g, 0.5 * (fresh_sq - fresh_mean * fresh_mean))
    rstd_g = lax.rsqrt(var_g + EPS)
    ids = lax.broadcasted_iota(jnp.int32, (groups, channels), 0).astype(F32)
    member_all = (gmap[0:1] == ids).astype(F32)
    scale = jnp.sum(member_all * rstd_g, axis=0, keepdims=True) * gamma_ref[...].reshape(1, channels)
    shift = beta_ref[...].reshape(1, channels) - (
        jnp.sum(member_all * mean_g, axis=0, keepdims=True) * scale
    )
    for k, vector in enumerate((scale, shift)):
        for j in range(channels // LANES):
            span = slice(j * LANES, (j + 1) * LANES)
            affine[k, span, :] = spread(0.5 * vector[:, span])

    img_copies = []
    for d in range(1, n_strip):
        peer = lax.rem(strip + d, n_strip)
        img_copies.append(
            send(st_strip, st_all.at[d], img_send.at[d], img_recv.at[d], (peer, me))
        )

    for slot in (0, slots - 1):
        row_copy(slot, 0, me, me).wait_recv()
        arrive(slot)
    has_above = strip > 0
    has_below = strip < n_strip - 1
    for c in range(n_chan):
        span = pl.ds(c * local_c, local_c)
        pad[0, span] = jnp.where(has_above, ga[c, 0].astype(F32), 0.0).astype(BF16)
        below = jnp.where(has_below, ga[c, slots - 1].astype(F32), 0.0)
        pad[slots, span] = below.astype(BF16)
        pad[slots - 1, span] = jnp.where(length + 1 == slots - 1, below, 0.0).astype(BF16)

    def relay(slot):
        forward(slot)

        @pl.when(slot + WINDOW <= rows)
        def _():
            start_row(slot + WINDOW, 0)

    def activate(slot):
        arrive(slot)
        for c in range(n_chan):
            for at in range(0, local_c, CHUNK):
                span = pl.ds(c * local_c + at, CHUNK)
                h = ga[c, slot, pl.ds(at, CHUNK)].astype(F32) * affine[0, span] + affine[1, span]
                act = jnp.where(slot - 1 < length, h + h * jnp.tanh(h), 0.0)
                below = pad[slots, span].astype(F32)
                pad[slot, span] = jnp.where(slot == length + 1, below, act).astype(BF16)

    for copy in w_copies:
        copy.wait()
    relay(1)
    activate(1)
    depth = 2
    place = lane_iota((local_c, width))

    def from_left(y):
        return jnp.where(place == 0, 0.0, pltpu.roll(y, 1, 1))

    def from_right(y):
        return jnp.where(place == width - 1, 0.0, pltpu.roll(y, width - 1, 1))

    def step(t, carry):
        more = t < rows // depth - 1
        relay(2 * t + 2)

        @pl.when(more)
        def _():
            relay(2 * t + 3)

        activate(2 * t + 2)

        @pl.when(more)
        def _():
            activate(2 * t + 3)

        first = depth * t
        rhs = jnp.concatenate(
            [
                jnp.concatenate([pad[first + dy + k] for k in range(depth)], axis=1)
                for dy in range(3)
            ],
            axis=0,
        )
        y = []
        for dx in range(3):
            lhs = jnp.concatenate([ws[3 * dy + dx] for dy in range(3)], axis=1)
            y.append(jnp.dot(lhs, rhs, preferred_element_type=F32))
        for k in range(depth):
            span = slice(k * width, (k + 1) * width)
            total = from_left(y[0][:, span]) + y[1][:, span] + from_right(y[2][:, span])
            block = xl[first + k].astype(F32) + total
            out_ref[first + k] = jnp.where(first + k < length, block, 0.0).astype(BF16)
        return carry

    lax.fori_loop(0, rows // depth, step, 0)

    for copy in img_copies:
        copy.wait_recv()
    st_all[0] = st_strip[...]
    image = jnp.zeros((8, LANES), F32)
    for i in range(n_strip):
        image = image + st_all[lax.rem(strip - i + n_strip, n_strip)]
    stat_ref[...] = image / total_count

    for copy in sends:
        copy.wait_send()

    def drain(slot, carry):
        for kind in range(1, 2 + n_chips - 1):
            row_copy(slot, kind, partner, me).wait_send()
        return carry

    def drain_forward(slot, carry):
        for kind in range(1 + n_chips, 2 * n_chips):
            row_copy(slot, kind, partner, me).wait_send()
        return carry

    lax.fori_loop(1, rows + 1, drain, 0)
    lax.fori_loop(0, slots, drain_forward, 0)


def upsample_kernel(block_ref, stat_ref, out_ref, mean_ref, square_ref):
    depth, _, width = block_ref.shape
    source = lax.broadcasted_iota(jnp.int32, (width, 2 * width), 0)
    target = lax.broadcasted_iota(jnp.int32, (width, 2 * width), 1) // 2
    twice = (target == source).astype(F32).astype(BF16)
    for r in range(depth):
        wide = jnp.dot(block_ref[r], twice, preferred_element_type=F32).astype(BF16)
        out_ref[2 * r] = wide
        out_ref[2 * r + 1] = wide
    groups = mean_ref.shape[1]
    mean_ref[...] = stat_ref[0:1, 0:groups]
    square_ref[...] = stat_ref[1:2, 0:groups]


def per_device(
    n_strip,
    n_chan,
    activations,
    weight,
    gamma,
    beta,
    group_map,
    lengths,
    stale_edges,
    stale_mean,
    stale_square,
    old_mean,
    old_square,
):
    rows, width, local_c = activations.shape
    channels = weight.shape[1]
    groups = stale_mean.shape[0]
    slots = rows + 2
    n_chips = n_chan // 2
    kinds = 2 * n_chips
    total_count = float(n_strip * (3 * rows // 4) * width * (channels // groups))
    vmem = pl.BlockSpec(memory_space=pltpu.VMEM)
    hbm = pl.BlockSpec(memory_space=pl.ANY)
    dma = pltpu.SemaphoreType.DMA
    block, stat = pl.pallas_call(
        functools.partial(conv_kernel, n_strip, n_chan, total_count),
        out_shape=(
            jax.ShapeDtypeStruct((rows, local_c, width), BF16),
            jax.ShapeDtypeStruct((8, LANES), F32),
        ),
        in_specs=[hbm, hbm, vmem, vmem, vmem, pl.BlockSpec(memory_space=pltpu.SMEM), hbm,
                  vmem, vmem, vmem, vmem],
        out_specs=(vmem, vmem),
        scratch_shapes=[
            pltpu.VMEM((rows, local_c, width), BF16),
            pltpu.VMEM((2, local_c, width), BF16),
            pltpu.VMEM((9, local_c, channels), BF16),
            pltpu.VMEM((n_chan, slots, local_c, width), BF16),
            pltpu.VMEM((slots + 1, channels, width), BF16),
            pltpu.VMEM((8, LANES), F32),
            pltpu.VMEM((n_chan, 8, LANES), F32),
            pltpu.VMEM((8, LANES), F32),
            pltpu.VMEM((n_strip, 8, LANES), F32),
            pltpu.VMEM((2, channels, width), F32),
            dma((3,)),
            dma((3,)),
            dma((kinds, slots)),
            dma((kinds, slots)),
            dma((2, 1 + n_chips)),
            dma((n_chan,)),
            dma((n_chan,)),
            dma((n_strip,)),
            dma((n_strip,)),
        ],
        compiler_params=pltpu.CompilerParams(
            collective_id=0, has_side_effects=True, vmem_limit_bytes=56 * 2**20
        ),
        name="conv",
    )(
        jnp.transpose(activations, (0, 2, 1)),
        jnp.transpose(weight, (0, 2, 1)),
        gamma,
        beta,
        group_map,
        lengths,
        jnp.transpose(stale_edges, (0, 2, 1)),
        stale_mean.reshape(1, groups),
        stale_square.reshape(1, groups),
        old_mean,
        old_square,
    )
    whole = pl.BlockSpec((1, groups), lambda r: (0, 0))
    upsampled, mean, square = pl.pallas_call(
        upsample_kernel,
        grid=(rows // 4,),
        out_shape=(
            jax.ShapeDtypeStruct((2 * rows, local_c, 2 * width), BF16),
            jax.ShapeDtypeStruct((1, groups), F32),
            jax.ShapeDtypeStruct((1, groups), F32),
        ),
        in_specs=[
            pl.BlockSpec((4, local_c, width), lambda r: (r, 0, 0)),
            pl.BlockSpec((8, LANES), lambda r: (0, 0)),
        ],
        out_specs=(pl.BlockSpec((8, local_c, 2 * width), lambda r: (r, 0, 0)), whole, whole),
        name="upsample",
    )(block, stat)
    upsampled = jnp.transpose(upsampled, (0, 2, 1))
    return upsampled, mean.reshape(groups), square.reshape(groups)


def solution(mesh):
    in_specs = (
        P("strip", None, "chan"),
        P(None, None, "chan"),
        P(),
        P(),
        P(),
        P("strip"),
        P("strip", None, "chan"),
        P(),
        P(),
        P("strip", None),
        P("strip", None),
    )
    out_specs = (P("strip", None, "chan"), P(), P())
    body = functools.partial(per_device, mesh.shape["strip"], mesh.shape["chan"])
    return jax.shard_map(
        body, mesh=mesh, in_specs=in_specs, out_specs=out_specs, check_vma=False
    )
```
